128 devices in a mesh: expert: 4 (over y_hi, core), shard: 32 (over z, y_lo, x).
Axes of the slice: x: 4, y: 4 (y_hi: 2, y_lo: 2; y = y_hi * 2 + y_lo), z: 4, core: 2. Of those that a mesh axis runs over, the one named last changes fastest.
Arguments:
- w_gate: float32 [128, 2048, 768], P('expert', 'shard'), may hold values from -0.25 to 0.25
- w_up: float32 [128, 2048, 768], P('expert', 'shard'), may hold values from -0.25 to 0.25
- router_weight: float32 [2048, 128], P('shard', 'expert'), may hold values from -0.125 to 0.125
- router_gain: float32 [2048], P('shard'), may hold values from 0.25 to 1.75
Outputs:
- serve_gate: bfloat16 [128, 2048, 768], P('expert', None, 'shard')
- serve_up: bfloat16 [128, 2048, 768], P('expert', None, 'shard')
- scale_gate: float32 [128, 768], P('expert', 'shard')
- scale_up: float32 [128, 768], P('expert', 'shard')
- serve_router: bfloat16 [2048, 128], replicated
The draws below stay inside these ranges and needn't reach their ends.
All inputs are finite; a program needn't handle non-finite values. Where the reference program divides by a largest or mean magnitude, that divisor is 1e-20 or more.
Results may differ from the reference program's by a relative error of at most 0.001.
Values may be sent and summed in bfloat16 or wider, within the bound.
A program may use at most 128 MiB of HBM per device.

```python
import jax
import jax.numpy as jnp

EXPERTS = 128
D_MODEL = 2048
D_EXPERT = 768


def with_spikes(result, stream_key, source, target, blocks, factor):
    def block_of(dim):
        return (jnp.arange(result.shape[dim]) // (result.shape[dim] // blocks)).reshape((-1,) + (1,) * (result.ndim - 1 - dim))

    near = jax.random.permutation(stream_key, blocks)[block_of(target)]
    other_side = (block_of(target) + blocks // 2) % blocks
    return jnp.where((block_of(source) == near) | (block_of(source) == other_side), factor * result, result)


def block_levels(rng, shape, cuts, low, largest):
    loudness, own = 1.0, jax.random.fold_in(rng, 6)
    for dim, blocks in cuts:
        steps = jnp.exp(jax.random.uniform(jax.random.fold_in(own, dim), (blocks,), jnp.float32, low / len(cuts), largest / len(cuts)))
        loudness = loudness * jnp.repeat(steps, shape[dim] // blocks).reshape([-1 if axis == dim else 1 for axis in range(len(shape))])
    return loudness


def normal_values(key, shape, deviation, reach, split=(), kind=jnp.bfloat16):
    loudness = block_levels(key, shape, split, -0.22, 0.18) if split else 1.0
    result = jax.random.normal(key, shape, jnp.float32) * deviation * loudness
    return jnp.minimum(jnp.maximum(result, -reach), reach).astype(kind)


def bell_draw_with(key, dims, width, most, cuts, heavy, dtype=jnp.bfloat16):
    result = width * jax.random.normal(key, dims, jnp.float32)
    if cuts:
        result = result * block_levels(key, dims, cuts, -0.22, 0.18)
    return jnp.clip(with_spikes(result, jax.random.fold_in(key, 3), *heavy), -most, most).astype(dtype)


def setup_inputs(seed: int = 0) -> dict:
    arg_keys = jax.random.split(jax.random.key(seed), 5)
    w_gate = bell_draw_with(arg_keys[0], (EXPERTS, D_MODEL, D_EXPERT), D_MODEL ** -0.5, 0.25, ((0, 4), (1, 32)), (1, 2, 32, 2.75), jnp.float32)
    w_up = bell_draw_with(arg_keys[1], (EXPERTS, D_MODEL, D_EXPERT), D_MODEL ** -0.5, 0.25, ((0, 4), (1, 32)), (1, 2, 32, 2.75), jnp.float32)
    router_weight = normal_values(arg_keys[2], (D_MODEL, EXPERTS), D_MODEL ** -0.5, 0.125, ((0, 32), (1, 4)), jnp.float32)
    router_gain = jnp.clip(1.0 + 0.15 * jax.random.normal(arg_keys[3], (D_MODEL,), jnp.float32), 0.25, 1.75)
    return dict(w_gate=w_gate, w_up=w_up, router_weight=router_weight, router_gain=router_gain)


def reference(w_gate, w_up, router_weight, router_gain):
    scale_gate = jnp.max(jnp.abs(w_gate), axis=1)
    serve_gate = (w_gate / jnp.expand_dims(scale_gate, 1)).astype(jnp.bfloat16)
    scale_up = jnp.max(jnp.abs(w_up), axis=1)
    serve_up = (w_up / jnp.expand_dims(scale_up, 1)).astype(jnp.bfloat16)
    serve_router = (router_weight * router_gain[:, None]).astype(jnp.bfloat16)
    return serve_gate, serve_up, scale_gate, scale_up, serve_router
```

```python
import functools

import jax
import jax.numpy as jnp
from jax import lax
from jax.experimental import pallas as pl
from jax.experimental.pallas import tpu as pltpu
from jax.sharding import PartitionSpec as P

MESH = pl.DeviceIdType.MESH
N = 32
CHUNKS = 8
PAIRS = 4
COLS = 24

SLOTS = (
    ((1, 1, 1), (3, 0, 3)),
    ((1, 0, 1), (3, 1, 3)),
    ((1, 1, 3), (3, 0, 1)),
    ((1, 0, 3), (3, 1, 1)),
    ((2, 1, 2),),
    ((2, 0, 2), (0, 1, 0)),
    ((2, 1, 0), (0, 0, 2)),
    ((2, 0, 0), (0, 1, 2)),
    ((2, 1, 1), (0, 0, 3)),
    ((2, 0, 1), (0, 1, 3)),
    ((2, 0, 3), (0, 1, 1)),
    ((2, 1, 3), (0, 0, 1)),
    ((1, 1, 2), (3, 0, 0)),
    ((1, 0, 2), (3, 1, 0)),
    ((3, 0, 2), (1, 1, 0)),
    ((3, 1, 2), (1, 0, 0)),
)
OFFSETS = tuple(o for slot in SLOTS for o in slot)


def partner(me, offset):
    dz, dy, dx = offset
    z, y, x = me // 8, lax.rem(me // 4, 2), lax.rem(me, 4)
    return lax.rem(z + dz, 4) * 8 + lax.rem(y + dy, 2) * 4 + lax.rem(x + dx, 4)


def exchange(
    gate, up, router, gain,
    recv, scale_g, scale_u, rout,
    wbuf, send, lmax, rsbuf, scall, inv, tmp0, tmp1, rtile, rgot, rhalf, rbig,
    load_sem, rs_send, rs_recv, ag_send, ag_recv, r1_send, r1_recv, r2_send, r2_recv, r3_send, r3_recv,
    a_send, a_recv, own_sem, rown_sem,
):
    me = lax.axis_index("shard")
    e = lax.axis_index("expert")
    core = lax.rem(e, 2)

    def load(c):
        src = gate if c < CHUNKS // 2 else up
        row = c % (CHUNKS // 2) * PAIRS
        return pltpu.make_async_copy(
            src.at[pl.ds(row, PAIRS)], wbuf.at[pl.ds(c * PAIRS, PAIRS)], load_sem.at[c]
        )

    for c in range(CHUNKS):
        load(c).start()

    barrier = pltpu.get_barrier_semaphore()
    for o in OFFSETS:
        pl.semaphore_signal(barrier, inc=1, device_id={"shard": partner(me, o)}, device_id_type=MESH)
    for k in range(1, 4):
        pl.semaphore_signal(barrier, inc=1, device_id={"expert": lax.rem(e + k, 4)}, device_id_type=MESH)

    part = router[...] * gain[...]
    for k in range(4):
        rbig[pl.ds(32 * k, 32), pl.ds(0, 64)] = part
    tile = rbig[...].T[:64].astype(jnp.bfloat16)
    rtile[...] = tile
    rgot[e] = tile

    pl.semaphore_wait(barrier, len(OFFSETS) + 3)

    def r1(k):
        return pltpu.make_async_remote_copy(
            src_ref=rtile, dst_ref=rgot.at[e], send_sem=r1_send.at[k - 1], recv_sem=r1_recv.at[k - 1],
            device_id={"expert": lax.rem(e + k, 4)}, device_id_type=MESH,
        )

    for k in range(1, 4):
        r1(k).start()

    for c in range(CHUNKS):
        load(c).wait()

        def pair_max(q, carry, c=c):
            p = c * PAIRS + q
            for h in range(2):
                for j in range(6):
                    block = wbuf[p, pl.ds(64 * h, 64), pl.ds(128 * j, 128)]
                    lmax[p, pl.ds(6 * h + j, 1), :] = jnp.max(jnp.abs(block), axis=0, keepdims=True)

            @pl.when(p != me)
            def _():
                pltpu.make_async_remote_copy(
                    src_ref=lmax.at[p], dst_ref=rsbuf.at[me], send_sem=rs_send, recv_sem=rs_recv,
                    device_id={"shard": p}, device_id_type=MESH,
                ).start()

            return carry

        lax.fori_loop(0, PAIRS, pair_max, 0)

    rsbuf[me] = lmax[me]
    others = pl.ds(0, N - 1)
    pltpu.make_async_copy(rsbuf.at[others], rsbuf.at[others], rs_recv).wait()
    scall[me] = lax.fori_loop(1, N, lambda s, m: jnp.maximum(m, rsbuf[s]), rsbuf[0])
    for o in OFFSETS:
        pltpu.make_async_remote_copy(
            src_ref=scall.at[me], dst_ref=scall.at[me], send_sem=ag_send, recv_sem=ag_recv.at[me],
            device_id={"shard": partner(me, o)}, device_id_type=MESH,
        ).start()

    for k in range(1, 4):
        r1(k).wait_recv()
    lane = lax.broadcasted_iota(jnp.int32, (32, 128), 1) // 32
    rows = pl.ds(pl.multiple_of(core * 32, 32), 32)
    wide = [rgot[k, rows, :].astype(jnp.float32) for k in range(4)]
    merged = jnp.where(lane == 0, wide[0], jnp.where(lane == 1, wide[1], jnp.where(lane == 2, wide[2], wide[3])))
    rhalf[...] = merged.astype(jnp.bfloat16)
    rown = pltpu.make_async_copy(rhalf, rout.at[me, core], rown_sem)
    rown.start()
    for o in OFFSETS:
        pltpu.make_async_remote_copy(
            src_ref=rhalf, dst_ref=rout.at[me, core], send_sem=r2_send, recv_sem=r2_recv,
            device_id={"shard": partner(me, o)}, device_id_type=MESH,
        ).start()

    def chunk(c, carry):
        for q in range(PAIRS):
            p = c * PAIRS + q

            @pl.when(p != me)
            def _():
                pltpu.make_async_copy(scall.at[p], scall.at[p], ag_recv.at[p]).wait()

        def pair(q, carry):
            p = c * PAIRS + q
            inv[...] = 1.0 / scall[p]
            for j in range(6):
                cols = pl.ds(128 * j, 128)
                top = wbuf[p, pl.ds(0, 64), cols] * inv[pl.ds(j, 1), :]
                low = wbuf[p, pl.ds(64, 64), cols] * inv[pl.ds(6 + j, 1), :]
                block = jnp.concatenate([top, low], axis=0)
                send[c, q, cols, :] = block.T.astype(jnp.bfloat16)
            return carry

        lax.fori_loop(0, PAIRS, pair, 0)

        def mine(d):
            return send.at[c, :, pl.ds(pl.multiple_of(d * COLS, 8), COLS), :]

        pltpu.make_async_copy(mine(me), recv.at[c, me], own_sem.at[c]).start()
        for o in OFFSETS:
            d = partner(me, o)
            pltpu.make_async_remote_copy(
                src_ref=mine(d), dst_ref=recv.at[c, me], send_sem=a_send.at[c], recv_sem=a_recv.at[c],
                device_id={"shard": d}, device_id_type=MESH,
            ).start()
        return carry

    lax.fori_loop(0, CHUNKS, chunk, 0)

    first = me * COLS
    j0, off = first // 128, lax.rem(first, 128)
    j1 = jnp.minimum(j0 + 1, 5)

    def pick(r, carry):
        p, h = r // 2, lax.rem(r, 2)
        tmp0[pl.ds(r, 1), :] = scall[p, pl.ds(h * 6 + j0, 1), :]
        tmp1[pl.ds(r, 1), :] = scall[p, pl.ds(h * 6 + j1, 1), :]
        return carry

    lax.fori_loop(0, 64, pick, 0)
    back = lax.rem(128 - off, 128)
    where = lax.broadcasted_iota(jnp.int32, (128, 128), 1) < 128 - off
    own = jnp.where(where, pltpu.roll(tmp0[...], back, 1), pltpu.roll(tmp1[...], back, 1)).T
    scale_g[...] = own[:COLS, 0:32]
    scale_u[...] = own[:COLS, 32:64]

    rown.wait()
    half = rout.at[pl.ds(0, N - 1), 0]
    pltpu.make_async_copy(half, half, r2_recv).wait()
    r3 = pltpu.make_async_remote_copy(
        src_ref=rout.at[:, core], dst_ref=rout.at[:, core], send_sem=r3_send, recv_sem=r3_recv,
        device_id={"expert": e + 1 - 2 * core}, device_id_type=MESH,
    )
    r3.start()

    pltpu.make_async_copy(rsbuf.at[others], rsbuf.at[others], rs_send).wait()
    pltpu.make_async_copy(rsbuf.at[others], rsbuf.at[others], ag_send).wait()
    for k in range(1, 4):
        r1(k).wait_send()
    pltpu.make_async_copy(half, half, r2_send).wait()
    for c in range(CHUNKS):
        pltpu.make_async_copy(recv.at[c, 0], recv.at[c, 0], own_sem.at[c]).wait()
        pltpu.make_async_copy(recv.at[c, others], recv.at[c, others], a_send.at[c]).wait()
        pltpu.make_async_copy(recv.at[c, others], recv.at[c, others], a_recv.at[c]).wait()
    r3.wait()


def merge(recv, sg, su, router, gate, up, og, ou, orouter):
    c = pl.program_id(0)

    def into(out):
        low = lax.broadcasted_iota(jnp.int32, (COLS, 128), 1) < 64
        for q in range(PAIRS):
            for k in range(N // 2):
                a = recv[0, 2 * k, q].astype(jnp.float32)
                b = recv[0, 2 * k + 1, q].astype(jnp.float32)
                lanes = pl.ds(128 * k, 128)
                out[2 * q, :, lanes] = jnp.where(low, a, pltpu.roll(b, 64, 1)).astype(jnp.bfloat16)
                out[2 * q + 1, :, lanes] = jnp.where(low, pltpu.roll(a, 64, 1), b).astype(jnp.bfloat16)

    @pl.when(c < CHUNKS // 2)
    def _():
        into(gate)

    @pl.when(c >= CHUNKS // 2)
    def _():
        into(up)

    orouter[...] = router[...]

    @pl.when(c == 0)
    def _():
        og[...] = sg[...]
        ou[...] = su[...]


def body(w_gate, w_up, router_weight, router_gain):
    f32, bf16 = jnp.float32, jnp.bfloat16
    hbm, vmem = pl.BlockSpec(memory_space=pltpu.HBM), pl.BlockSpec(memory_space=pltpu.VMEM)
    dma = pltpu.SemaphoreType.DMA
    recv, sg, su, rout = pl.pallas_call(
        exchange,
        out_shape=(
            jax.ShapeDtypeStruct((CHUNKS, N, PAIRS, COLS, 128), bf16),
            jax.ShapeDtypeStruct((COLS, 32), f32),
            jax.ShapeDtypeStruct((COLS, 32), f32),
            jax.ShapeDtypeStruct((N, 2, 32, 128), bf16),
        ),
        in_specs=[hbm, hbm, vmem, vmem],
        out_specs=(hbm, vmem, vmem, hbm),
        scratch_shapes=[
            pltpu.VMEM((N, 128, 768), f32),
            pltpu.VMEM((CHUNKS, PAIRS, 768, 128), bf16),
            pltpu.VMEM((N, 12, 128), f32),
            pltpu.VMEM((N, 12, 128), f32),
            pltpu.VMEM((N, 12, 128), f32),
            pltpu.VMEM((12, 128), f32),
            pltpu.VMEM((128, 128), f32),
            pltpu.VMEM((128, 128), f32),
            pltpu.VMEM((64, 128), bf16),
            pltpu.VMEM((4, 64, 128), bf16),
            pltpu.VMEM((32, 128), bf16),
            pltpu.VMEM((128, 128), f32),
            dma((CHUNKS,)), dma, dma, dma, dma((N,)), dma((3,)), dma((3,)), dma, dma, dma, dma,
            dma((CHUNKS,)), dma((CHUNKS,)), dma((CHUNKS,)), dma,
        ],
        compiler_params=pltpu.CompilerParams(
            collective_id=0, has_side_effects=True, vmem_limit_bytes=62 * 2**20
        ),
        name="exchange",
    )(
        w_gate.reshape(16, 128, 768),
        w_up.reshape(16, 128, 768),
        router_weight.T,
        router_gain.reshape(1, 64),
    )
    last = CHUNKS // 2 - 1
    gate, up, sg, su, router = pl.pallas_call(
        merge,
        grid=(CHUNKS,),
        out_shape=(
            jax.ShapeDtypeStruct((32, COLS, 2048), bf16),
            jax.ShapeDtypeStruct((32, COLS, 2048), bf16),
            jax.ShapeDtypeStruct((COLS, 32), f32),
            jax.ShapeDtypeStruct((COLS, 32), f32),
            jax.ShapeDtypeStruct((2048, 128), bf16),
        ),
        in_specs=[
            pl.BlockSpec((1, N, PAIRS, COLS, 128), lambda c: (c, 0, 0, 0, 0)),
            pl.BlockSpec((COLS, 32), lambda c: (0, 0)),
            pl.BlockSpec((COLS, 32), lambda c: (0, 0)),
            pl.BlockSpec((256, 128), lambda c: (c, 0)),
        ],
        out_specs=(
            pl.BlockSpec((8, COLS, 2048), lambda c: (jnp.minimum(c, last), 0, 0)),
            pl.BlockSpec((8, COLS, 2048), lambda c: (jnp.maximum(c - last - 1, 0), 0, 0)),
            pl.BlockSpec((COLS, 32), lambda c: (0, 0)),
            pl.BlockSpec((COLS, 32), lambda c: (0, 0)),
            pl.BlockSpec((256, 128), lambda c: (c, 0)),
        ),
        name="merge",
    )(recv, sg, su, rout.reshape(2048, 128))
    return (gate.swapaxes(1, 2), up.swapaxes(1, 2), sg.T, su.T, router)


def solution(mesh):
    return jax.shard_map(
        body,
        mesh=mesh,
        in_specs=(
            P("expert", "shard", None),
            P("expert", "shard", None),
            P("shard", "expert"),
            P("shard"),
        ),
        out_specs=(
            P("expert", None, "shard"),
            P("expert", None, "shard"),
            P("expert", "shard"),
            P("expert", "shard"),
            P(),
        ),
        check_vma=False,
    )
```
